32 devices in a mesh: clip: 2 (over y), tm: 4 (over z), space: 2 (over x), chan: 2 (over core).
Axes of the slice: x: 2, y: 2, z: 4, core: 2. Of those that a mesh axis runs over, the one named last changes fastest.
Arguments:
- features: bfloat16 [16, 8, 90, 256], P(('clip', 'tm'), 'space'), parts along dimension 0, may hold values from -700 to 700
- hidden: bfloat16 [16, 8, 90, 256], P(('clip', 'tm'), 'space'), parts along dimension 0, may hold values from -700 to 700
- cotangent: bfloat16 [16, 8, 90, 256], P(('clip', 'tm'), 'space'), parts along dimension 0, may hold values from -6 to 6
- kernel_one: bfloat16 [256, 3, 3, 3, 256], P(None, None, None, None, 'chan'), may hold values from -0.078125 to 0.078125
- kernel_two: bfloat16 [256, 3, 3, 3, 256], P(None, None, None, None, 'chan'), may hold values from -0.078125 to 0.078125
- gains: float32 [2, 256], replicated, may hold values from 0.25 to 1.75
Outputs:
- feature_grad: bfloat16 [16, 8, 90, 256], P(('clip', 'tm'), 'space', None, 'chan'), parts along dimension 0
- delta_one: float32 [512, 3, 3, 3, 256], P(('clip', 'tm', 'space'), None, None, None, 'chan'), parts along dimension 0
- delta_two: float32 [512, 3, 3, 3, 256], P(('clip', 'tm', 'space'), None, None, None, 'chan'), parts along dimension 0
- gain_grads: float32 [4, 256], P('clip', 'chan'), parts along dimension 0
The draws below stay inside these ranges and needn't reach their ends.
There are 2 independent parts, one for each index of `clip`. The reference program is written for one: setup_inputs(seed, part) draws one part's arguments, and reference() takes and returns one part's arrays. A program takes and returns all parts, laid end to end along the dimension named above; an argument that names none is the same for every part. Nothing has to cross between parts.
All inputs are finite; a program needn't handle non-finite values.
Results may differ from the reference program's by a relative error of at most 0.005.
Values may be sent and summed in bfloat16 or wider, within the bound.
A program may use at most 128 MiB of HBM per device.

```python
import math
import jax
import jax.numpy as jnp
from jax import lax

C = 256
GROUPS = 32
W = 90
FRAMES = 8
HEIGHT = 8


def field_draw(key):
    key_base, key_rows, key_chan = jax.random.split(key, 3)
    shape = (FRAMES, HEIGHT, W, C)
    row_scale = 0.2 * jnp.exp(jax.random.uniform(key_rows, (FRAMES, HEIGHT, 1, 1), jnp.float32, 0.0, math.log(10.0)))
    chan_scale = jnp.exp(jax.random.uniform(key_chan, (1, 1, 1, C), jnp.float32, 0.0, math.log(4.0)))
    position = jnp.arange(FRAMES, dtype=jnp.float32).reshape(FRAMES, 1, 1, 1) / max(FRAMES - 1, 1)
    base = jnp.clip(jax.random.normal(key_base, shape, jnp.float32), -4.0, 4.0)
    rise = jnp.exp(0.5 * math.log(3.0) * position)
    return base * row_scale * chan_scale * rise


def draw_features(key, part):
    return field_draw(jax.random.fold_in(key, 11)).astype(jnp.bfloat16)


def draw_hidden(key, part):
    return field_draw(jax.random.fold_in(key, 23)).astype(jnp.bfloat16)


def block_levels(rng, shape, cuts, least, high):
    loudness, own = 1.0, jax.random.fold_in(rng, 6)
    for dim, blocks in cuts:
        heights = jnp.exp(jax.random.uniform(jax.random.fold_in(own, dim), (blocks,), jnp.float32, least / len(cuts), high / len(cuts)))
        loudness = loudness * jnp.repeat(heights, shape[dim] // blocks).reshape([-1 if axis == dim else 1 for axis in range(len(shape))])
    return loudness


def scatter_about(stream_key, extent, deviation, bound, cuts=(), kind=jnp.bfloat16):
    entries = deviation * jax.random.normal(stream_key, extent, jnp.float32)
    if cuts:
        entries = entries * block_levels(stream_key, extent, cuts, -0.22, 0.18)
    return jnp.clip(entries, -bound, bound).astype(kind)


def setup_inputs(seed: int = 0, part: int = 0) -> dict:
    streams_of = jax.random.split(jax.random.key(seed), 7)
    part_splits = jax.random.split(jax.random.fold_in(streams_of[6], part), 7)
    features = draw_features(jax.random.fold_in(jax.random.fold_in(streams_of[6], part), 71), part)
    hidden = draw_hidden(jax.random.fold_in(jax.random.fold_in(streams_of[6], part), 71), part)
    cotangent = scatter_about(part_splits[2], (FRAMES, HEIGHT, W, C), 1.0, 6.0, ((0, 4), (1, 2)))
    kernel_one = scatter_about(streams_of[3], (C, 3, 3, 3, C), (27 * C) ** -0.5, 0.078125, ((4, 2),))
    kernel_two = scatter_about(streams_of[4], (C, 3, 3, 3, C), (27 * C) ** -0.5, 0.078125, ((4, 2),))
    gains = jnp.clip(1.0 + 0.15 * jax.random.normal(streams_of[5], (2, C), jnp.float32), 0.25, 1.75)
    return dict(features=features, hidden=hidden, cotangent=cotangent, kernel_one=kernel_one, kernel_two=kernel_two, gains=gains)


epsilon = 1e-06

def moments(field, gain, members):
    per = field.shape[3] // GROUPS
    total = lax.optimization_barrier(jnp.sum(field, axis=(0, 1, 2))).reshape(GROUPS, per)
    square = lax.optimization_barrier(jnp.sum(field * field, axis=(0, 1, 2))).reshape(GROUPS, per)
    mean = lax.optimization_barrier(jnp.sum(total, axis=1)) / members
    spread = lax.optimization_barrier(jnp.sum(square, axis=1)) / members - mean * mean
    scale = jnp.repeat(lax.rsqrt(spread + epsilon), per)
    centred = (field - jnp.repeat(mean, per)) * scale
    return (centred, centred * gain, scale)

def norm_back(upstream, centred, scaled, gain, scale, members):
    per = upstream.shape[3] // GROUPS
    gate = jax.nn.sigmoid(scaled)
    slope = upstream * gate * (1.0 + scaled * (1.0 - gate))
    plain = lax.optimization_barrier(jnp.sum(slope, axis=(0, 1, 2)))
    weighted = lax.optimization_barrier(jnp.sum(slope * centred, axis=(0, 1, 2)))
    first = jnp.repeat(lax.optimization_barrier(jnp.sum((gain * plain).reshape(-1, per), axis=1)), per) / members
    second = jnp.repeat(lax.optimization_barrier(jnp.sum((gain * weighted).reshape(-1, per), axis=1)), per) / members
    return (scale * (slope * gain - first - centred * second), weighted)

def conv_back(active, grad, kernel):
    frames, height, width, channels = active.shape
    padded = jnp.pad(grad.astype(jnp.float32), ((0, 2), (1, 1), (1, 1), (0, 0)))
    flipped = jnp.flip(jnp.transpose(kernel.astype(jnp.float32), (1, 2, 3, 4, 0)), (0, 1, 2))
    back = lax.conv_general_dilated(padded[None], flipped, (1, 1, 1), ((0, 0), (0, 0), (0, 0)), dimension_numbers=('NDHWC', 'DHWIO', 'NDHWC'), precision=lax.Precision.HIGHEST)[0]
    flat = active.reshape(-1, channels).astype(jnp.float32)
    pieces = []
    for frame_tap in range(3):
        for row_tap in range(3):
            for col_tap in range(3):
                window = padded[2 - frame_tap:2 - frame_tap + frames, 2 - row_tap:2 - row_tap + height, 2 - col_tap:2 - col_tap + width].reshape(-1, channels)
                pieces.append(lax.dot_general(flat, window, (((0,), (0,)), ((), ())), precision=lax.Precision.HIGHEST))
    delta = jnp.stack(pieces, axis=1).reshape(channels, 3, 3, 3, channels)
    return (delta, back)

def reference(features, hidden, cotangent, kernel_one, kernel_two, gains):
    members = float(FRAMES * HEIGHT * W * (C // GROUPS))
    centred_one, scaled_one, scale_one = moments(features.astype(jnp.float32), gains[0], members)
    centred_two, scaled_two, scale_two = moments(hidden.astype(jnp.float32), gains[1], members)
    active_one = (scaled_one * jax.nn.sigmoid(scaled_one)).astype(jnp.bfloat16)
    active_two = (scaled_two * jax.nn.sigmoid(scaled_two)).astype(jnp.bfloat16)
    delta_two, back_two = conv_back(active_two, cotangent, kernel_two)
    grad_two, weighted_two = norm_back(back_two, centred_two, scaled_two, gains[1], scale_two, members)
    grad_hidden = grad_two.astype(jnp.bfloat16)
    delta_one, back_one = conv_back(active_one, grad_hidden, kernel_one)
    grad_one, weighted_one = norm_back(back_one, centred_one, scaled_one, gains[0], scale_one, members)
    feature_grad = (cotangent.astype(jnp.float32) + grad_one).astype(jnp.bfloat16)
    return (feature_grad, delta_one, delta_two, jnp.stack([weighted_one, weighted_two]))
```

```python
import functools

import jax
import jax.numpy as jnp
from jax import lax
from jax.experimental import pallas as pl
from jax.experimental.pallas import tpu as pltpu
from jax.sharding import PartitionSpec as P

GROUPS = 32
EPS = 1e-06
MESH = pl.DeviceIdType.MESH
F32 = jnp.float32
BF16 = jnp.bfloat16


def group_sums(values, per):
    channels = values.shape[1]
    row = lax.broadcasted_iota(jnp.int32, (channels, channels), 0) // per
    col = lax.broadcasted_iota(jnp.int32, (channels, channels), 1) // per
    same = jnp.where(row == col, 1.0, 0.0).astype(F32)
    return jnp.dot(values, same, precision=lax.Precision.HIGHEST, preferred_element_type=F32)


def body(
    sizes,
    f_ref, h_ref, cot_ref, k1_ref, k2_ref, gain_ref,
    fg_ref, d1_ref, d2_ref, w_ref,
    ext2, ext1, gh, taps, act1, act2, acc,
    xs2, xr2, xs1, xr1, vec, r0, r2, r1, dd2, dd1, rr2, rr1,
    halo_s, halo_r, xsem_s, xsem_r, ar_s, ar_r, dl_s, dl_r,
):
    width, n_t, n_s = sizes
    frames, height, padded, half = cot_ref.shape
    channels = f_ref.shape[3]
    per = channels // GROUPS
    n = n_t * n_s
    rows = frames * height * padded
    block = height * padded
    share = channels // n
    t = lax.axis_index("tm")
    s = lax.axis_index("space")
    chan = lax.axis_index("chan")
    partner = 1 - chan
    rank = t * n_s + s
    members = float(frames * height * width * per * n)
    mine = pl.ds(pl.multiple_of(chan * half, half), half)
    theirs = pl.ds(pl.multiple_of(partner * half, half), half)

    def place(j):
        return {"tm": j // n_s, "space": lax.rem(j, n_s)}

    def peer(k):
        return lax.rem(rank + k, n)

    def each_peer(fn):
        def step(k, carry):
            fn(k)
            return carry

        lax.fori_loop(1, n, step, 0)

    ext2[...] = jnp.zeros_like(ext2)
    ext1[...] = jnp.zeros_like(ext1)

    barrier = pltpu.get_barrier_semaphore()
    pl.semaphore_signal(barrier, inc=1, device_id={"chan": partner}, device_id_type=MESH)
    each_peer(
        lambda k: pl.semaphore_signal(barrier, inc=1, device_id=place(peer(k)), device_id_type=MESH)
    )
    pl.semaphore_wait(barrier, n)

    last = height - 1
    below = (slice(0, frames), slice(height + 1, height + 2))
    above = (slice(0, frames), slice(0, 1))
    later = slice(frames, frames + 2)
    moves = (
        (0, -1, (slice(0, frames), slice(0, 1)), below),
        (0, 1, (slice(0, frames), slice(last, last + 1)), above),
        (-1, 0, (slice(0, 2), slice(0, height)), (later, slice(1, height + 1))),
        (-1, -1, (slice(0, 2), slice(0, 1)), (later, slice(height + 1, height + 2))),
        (-1, 1, (slice(0, 2), slice(last, last + 1)), (later, slice(0, 1))),
    )

    def inside(dt, ds):
        ok = None
        for value, step, count in ((t, dt, n_t), (s, ds, n_s)):
            if step:
                now = (value + step >= 0) & (value + step < count)
                ok = now if ok is None else ok & now
        return ok

    def halo(layer, source, dest, m):
        dt, ds, src, dst = moves[m]
        return pltpu.make_async_remote_copy(
            src_ref=source.at[src], dst_ref=dest.at[dst],
            send_sem=halo_s.at[layer, m], recv_sem=halo_r.at[layer, m],
            device_id={"tm": t + dt, "space": s + ds}, device_id_type=MESH,
        )

    def halo_start(layer, source, dest):
        for m in (2, 0, 1, 3, 4):
            @pl.when(inside(moves[m][0], moves[m][1]))
            def _(m=m):
                halo(layer, source, dest, m).start()

    def halo_arrive(layer, source, dest):
        for m in (2, 0, 1, 3, 4):
            @pl.when(inside(-moves[m][0], -moves[m][1]))
            def _(m=m):
                halo(layer, source, dest, m).wait_recv()

    def halo_end(layer, source, dest):
        for m in (2, 0, 1, 3, 4):
            @pl.when(inside(moves[m][0], moves[m][1]))
            def _(m=m):
                halo(layer, source, dest, m).wait_send()

    def sums_copy(layer, buf, k, slot):
        return pltpu.make_async_remote_copy(
            src_ref=buf.at[slot], dst_ref=buf.at[slot],
            send_sem=ar_s.at[layer, k], recv_sem=ar_r.at[layer, slot],
            device_id=place(peer(k)), device_id_type=MESH,
        )

    def sums_start(layer, buf, values):
        buf[rank] = values
        each_peer(lambda k: sums_copy(layer, buf, k, rank).start())

    def sums_finish(layer, buf):
        each_peer(lambda k: sums_copy(layer, buf, k, peer(k)).wait_recv())
        return jnp.sum(buf[...], axis=0)

    def sums_end(layer, buf):
        each_peer(lambda k: sums_copy(layer, buf, k, rank).wait_send())

    def share_copy(layer, out, buf, k, target, slot):
        return pltpu.make_async_remote_copy(
            src_ref=out.at[target], dst_ref=buf.at[slot],
            send_sem=dl_s.at[layer, k], recv_sem=dl_r.at[layer, slot],
            device_id=place(peer(k)), device_id_type=MESH,
        )

    def cross(layer, source, dest, f):
        return pltpu.make_async_remote_copy(
            src_ref=source.at[f], dst_ref=dest.at[f],
            send_sem=xsem_s.at[layer, f], recv_sem=xsem_r.at[layer, f],
            device_id={"chan": partner}, device_id_type=MESH,
        )

    column = lax.rem(lax.broadcasted_iota(jnp.int32, (rows, 1), 0), padded)
    real = column < width

    halo_start(0, cot_ref, ext2)
    ext2[0:frames, 1 : height + 1] = cot_ref[...]
    field_one = f_ref[...].reshape(rows, channels).astype(F32)
    field_two = h_ref[...].reshape(rows, channels).astype(F32)
    parts = [
        jnp.sum(field_one, axis=0, keepdims=True),
        jnp.sum(field_one * field_one, axis=0, keepdims=True),
        jnp.sum(field_two, axis=0, keepdims=True),
        jnp.sum(field_two * field_two, axis=0, keepdims=True),
        jnp.zeros((4, channels), F32),
    ]
    sums_start(0, r0, jnp.concatenate(parts, axis=0))

    def fill_taps(ext):
        def step(f, carry):
            cells = ext[f].reshape((height + 2) * padded, half).astype(F32)
            size = cells.shape[0]
            ahead = pltpu.roll(cells, size - 1, 0)
            behind = pltpu.roll(cells, 1, 0)
            for c, value in enumerate((ahead, cells, behind)):
                taps[f, :, :, c * half : (c + 1) * half] = value.astype(BF16).reshape(
                    height + 2, padded, half
                )
            return carry

        lax.fori_loop(0, frames + 2, step, 0)

    def conv(kernel, layer, source, dest):
        def step(f, carry):
            total = None
            for ab in range(9):
                a, b = ab // 3, ab % 3
                left = taps[2 - a + f, 2 - b : 2 - b + height].reshape(block, 3 * half)
                term = lax.dot_general(
                    left, kernel[ab], (((1,), (1,)), ((), ())), preferred_element_type=F32
                )
                total = term if total is None else total + term
            acc[f] = total
            source[f] = acc[f, :, theirs].astype(BF16)
            cross(layer, source, dest, f).start()
            return carry

        lax.fori_loop(0, frames, step, 0)

    def delta(act, out, own):
        def step(ab, carry):
            a = ab // 3
            b = lax.rem(ab, 3)
            right = taps[pl.ds(2 - a, frames), pl.ds(2 - b, height)].reshape(rows, 3 * half)
            product = jnp.dot(act[...], right, preferred_element_type=F32)
            small = product.astype(BF16)
            for j in range(n):
                out[j, ab] = small[j * share : (j + 1) * share]

                @pl.when(rank == j)
                def _(j=j):
                    own[ab] = product[j * share : (j + 1) * share]

            return carry

        lax.fori_loop(0, 9, step, 0)

    halo_arrive(0, cot_ref, ext2)
    fill_taps(ext2)
    conv(k2_ref, 0, xs2, xr2)

    totals = group_sums(sums_finish(0, r0), per) / members
    mean_one, mean_two = totals[0:1], totals[2:3]
    scale_one = lax.rsqrt(totals[1:2] - mean_one * mean_one + EPS)
    scale_two = lax.rsqrt(totals[3:4] - mean_two * mean_two + EPS)
    vec[0:1] = mean_one
    vec[1:2] = scale_one
    vec[2:3] = gain_ref[0:1]
    vec[3:4] = mean_two
    vec[4:5] = scale_two
    vec[5:6] = gain_ref[1:2]

    def activate(field_ref, base, act):
        field = field_ref[...].reshape(rows, channels).astype(F32)
        scaled = (field - vec[base : base + 1]) * vec[base + 1 : base + 2] * vec[base + 2 : base + 3]
        active = jnp.where(real, scaled * jax.nn.sigmoid(scaled), 0.0)
        act[...] = active.T.astype(BF16)

    activate(h_ref, 3, act2)
    delta(act2, dd2, d2_ref)

    def norm_back(field_ref, base, layer, dest, buf, w_row):
        for f in range(frames):
            cross(layer, xs2 if layer == 0 else xs1, dest, f).wait_recv()
        upstream = acc[:, :, mine].reshape(rows, half) + dest[...].reshape(rows, half).astype(F32)
        field = field_ref[:, :, :, mine].reshape(rows, half).astype(F32)
        scale = vec[base + 1 : base + 2, mine]
        gain = vec[base + 2 : base + 3, mine]
        centred = (field - vec[base : base + 1, mine]) * scale
        scaled = centred * gain
        gate = jax.nn.sigmoid(scaled)
        slope = jnp.where(real, upstream * gate * (1.0 + scaled * (1.0 - gate)), 0.0)
        parts = [
            jnp.sum(slope, axis=0, keepdims=True),
            jnp.sum(slope * centred, axis=0, keepdims=True),
            jnp.zeros((6, half), F32),
        ]
        sums_start(layer + 1, buf, jnp.concatenate(parts, axis=0))
        totals = sums_finish(layer + 1, buf)
        w_ref[w_row : w_row + 1] = totals[1:2]
        means = group_sums(totals * gain, per) / members
        grad = scale * (slope * gain - means[0:1] - centred * means[1:2])
        return jnp.where(real, grad, 0.0)

    grad_hidden = norm_back(h_ref, 3, 0, xr2, r2, 1).astype(BF16)
    gh[...] = grad_hidden.reshape(frames, height, padded, half)
    halo_start(1, gh, ext1)
    each_peer(lambda k: share_copy(0, dd2, rr2, k, peer(k), rank).start())
    ext1[0:frames, 1 : height + 1] = gh[...]
    activate(f_ref, 0, act1)
    halo_arrive(1, gh, ext1)
    fill_taps(ext1)
    conv(k1_ref, 1, xs1, xr1)
    delta(act1, dd1, d1_ref)
    each_peer(lambda k: share_copy(1, dd1, rr1, k, peer(k), rank).start())
    grad = norm_back(f_ref, 0, 1, xr1, r1, 0)
    fg_ref[...] = (cot_ref[...].reshape(rows, half).astype(F32) + grad).astype(BF16)

    def collect(layer, out, buf, own):
        def step(k, carry):
            share_copy(layer, out, buf, k, peer(k), peer(k)).wait_recv()
            own[...] += buf[peer(k)].astype(F32)
            return carry

        lax.fori_loop(1, n, step, 0)

    collect(0, dd2, rr2, d2_ref)
    collect(1, dd1, rr1, d1_ref)

    halo_end(0, cot_ref, ext2)
    halo_end(1, gh, ext1)
    sums_end(0, r0)
    sums_end(1, r2)
    sums_end(2, r1)
    for f in range(frames):
        cross(0, xs2, xr2, f).wait_send()
        cross(1, xs1, xr1, f).wait_send()
    each_peer(lambda k: share_copy(0, dd2, rr2, k, peer(k), rank).wait_send())
    each_peer(lambda k: share_copy(1, dd1, rr1, k, peer(k), rank).wait_send())


def shards(n_t, n_s, features, hidden, cotangent, kernel_one, kernel_two, gains):
    frames, height, width, channels = features.shape
    half = kernel_one.shape[4]
    padded = -(-width // 16) * 16
    if padded < width + 1:
        padded += 16
    n = n_t * n_s
    share = channels // n
    rows = frames * height * padded
    block = height * padded
    offset = lax.axis_index("chan") * half

    def wide(field):
        return jnp.pad(field, ((0, 0), (0, 0), (0, padded - width), (0, 0)))

    def stacked(kernel):
        return kernel.reshape(channels, 9, 3 * half).transpose(1, 0, 2)

    cot = wide(lax.dynamic_slice_in_dim(cotangent, offset, half, 3))
    vmem = pl.BlockSpec(memory_space=pltpu.VMEM)
    ext = pltpu.VMEM((frames + 2, height + 2, padded, half), BF16)
    halves = pltpu.VMEM((frames, block, half), BF16)
    pieces = pltpu.VMEM((n, 9, share, 3 * half), BF16)
    dma = pltpu.SemaphoreType.DMA
    grad, delta_one, delta_two, weighted = pl.pallas_call(
        functools.partial(body, (width, n_t, n_s)),
        out_shape=(
            jax.ShapeDtypeStruct((rows, half), BF16),
            jax.ShapeDtypeStruct((9, share, 3 * half), F32),
            jax.ShapeDtypeStruct((9, share, 3 * half), F32),
            jax.ShapeDtypeStruct((2, half), F32),
        ),
        in_specs=[vmem] * 6,
        out_specs=(vmem,) * 4,
        scratch_shapes=[
            ext,
            ext,
            pltpu.VMEM((frames, height, padded, half), BF16),
            pltpu.VMEM((frames + 2, height + 2, padded, 3 * half), BF16),
            pltpu.VMEM((channels, rows), BF16),
            pltpu.VMEM((channels, rows), BF16),
            pltpu.VMEM((frames, block, channels), F32),
            halves,
            halves,
            halves,
            halves,
            pltpu.VMEM((8, channels), F32),
            pltpu.VMEM((n, 8, channels), F32),
            pltpu.VMEM((n, 8, half), F32),
            pltpu.VMEM((n, 8, half), F32),
            pieces,
            pieces,
            pieces,
            pieces,
            dma((2, 5)),
            dma((2, 5)),
            dma((2, frames)),
            dma((2, frames)),
            dma((3, n)),
            dma((3, n)),
            dma((2, n)),
            dma((2, n)),
        ],
        compiler_params=pltpu.CompilerParams(
            collective_id=0, has_side_effects=True, vmem_limit_bytes=63 * 1024 * 1024
        ),
    )(wide(features), wide(hidden), cot, stacked(kernel_one), stacked(kernel_two), gains)

    def unstacked(delta):
        return delta.transpose(1, 0, 2).reshape(share, 3, 3, 3, half)

    feature_grad = grad.reshape(frames, height, padded, half)[:, :, :width]
    return (feature_grad, unstacked(delta_one), unstacked(delta_two), weighted)


def solution(mesh):
    placed = (
        P(("clip", "tm"), "space", None, None),
        P(("clip", "tm"), "space", None, None),
        P(("clip", "tm"), "space", None, None),
        P(None, None, None, None, "chan"),
        P(None, None, None, None, "chan"),
        P(),
    )
    return jax.shard_map(
        functools.partial(shards, mesh.shape["tm"], mesh.shape["space"]),
        mesh=mesh,
        in_specs=placed,
        out_specs=(
            P(("clip", "tm"), "space", None, "chan"),
            P(("clip", "tm", "space"), None, None, None, "chan"),
            P(("clip", "tm", "space"), None, None, None, "chan"),
            P("clip", "chan"),
        ),
        check_vma=False,
    )
```
